256 devices in a mesh: grp: 4 (over z_hi), dev: 64 (over x, z_lo, y, core).
Axes of the slice: x: 4, y: 4, z: 8 (z_hi: 4, z_lo: 2; z = z_hi * 2 + z_lo), core: 2. Of those that a mesh axis runs over, the one named last changes fastest.
Arguments:
- images: bfloat16 [12288, 1536], P(('grp', 'dev')), may hold values from -1 to 1, as said below
- texts: bfloat16 [12288, 1536], P(('grp', 'dev')), may hold values from -1 to 1, as said below
- logit_scale: float32 [1], replicated, may hold values from 20 to 60
- logit_bias: float32 [1], replicated, may hold values from -12 to -8
Outputs:
- grad_image: float32 [12288, 1536], P(('grp', 'dev'))
- grad_text: float32 [12288, 1536], P(('grp', 'dev'))
- loss: float32 [1], replicated
The draws below stay inside these ranges and needn't reach their ends.
Inputs may be any that keep to these rules, and one draw needn't show every extreme that they name: `images`: every row has length 1 up to bfloat16 rounding. `texts`: every row has length 1 up to bfloat16 rounding.
All inputs are finite; a program needn't handle non-finite values.
Results may differ from the reference program's by a relative error of at most 0.00095.
Values may be sent and summed in bfloat16 or wider, within the bound.
No kernel may reach another device: no remote copies, remote signals or barrier semaphores. Data moves between devices by JAX's collectives and lax.ppermute only.
A program may use at most 128 MiB of HBM per device.

```python
import jax
import jax.numpy as jnp
from jax import lax

D = 1536
ROWS = 48
BATCH = 12288
N_DEV = 64


def unit_rows(values):
    return values / jnp.sqrt(jnp.sum(values * values, axis=-1, keepdims=True))


def paired_rows(key):
    spread = 0.65
    column_scale = jnp.exp(spread * jax.random.normal(jax.random.fold_in(key, 11), (D,), jnp.float32))
    image_raw = jax.random.normal(jax.random.fold_in(key, 12), (BATCH, D), jnp.float32)
    noise_raw = jax.random.normal(jax.random.fold_in(key, 13), (BATCH, D), jnp.float32)
    image_dir = unit_rows(image_raw * column_scale[None, :])
    noise_dir = unit_rows(noise_raw * column_scale[None, :])
    text_dir = unit_rows(0.8 * image_dir + 0.6 * noise_dir)
    return (image_dir, text_dir)


def draw_images(key, part):
    return paired_rows(key)[0].astype(jnp.bfloat16)


def draw_texts(key, part):
    return paired_rows(key)[1].astype(jnp.bfloat16)


def setup_inputs(seed: int = 0) -> dict:
    key_list = jax.random.split(jax.random.key(seed), 5)
    return {
        "images": draw_images(jax.random.fold_in(key_list[4], 71), 0),
        "texts": draw_texts(jax.random.fold_in(key_list[4], 71), 0),
        "logit_scale": jnp.clip(jax.random.uniform(key_list[2], (1,), jnp.float32, 20.0, 60.0), 20.0, 60.0),
        "logit_bias": jnp.clip(jax.random.uniform(key_list[3], (1,), jnp.float32, -12.0, -8.0), -12.0, -8.0),
    }


def reference(images, texts, logit_scale, logit_bias):
    logit_mult = logit_scale[0]
    logit_shift = logit_bias[0]
    pair_total = images.shape[0]
    block_rows = N_DEV * ROWS
    block_number = pair_total // block_rows
    text_ids = jnp.arange(pair_total, dtype=jnp.int32)

    def block_step(running, block_index):
        grad_texts, loss_sum = running
        first_row = (block_index * block_rows).astype(jnp.int32)
        left_rows = lax.dynamic_slice_in_dim(images, first_row, block_rows, 0)
        left_ids = first_row + jnp.arange(block_rows, dtype=jnp.int32)
        logits = jnp.dot(left_rows, texts.T, preferred_element_type=jnp.float32) * logit_mult + logit_shift
        matched = left_ids[:, None] == text_ids[None, :]
        labels = jnp.where(matched, 1.0, -1.0).astype(jnp.float32)
        loss_part = -jnp.sum(jax.nn.log_sigmoid(labels * logits))
        weights = (jax.nn.sigmoid(logits) - matched.astype(jnp.float32)).astype(jnp.bfloat16)
        grad_left = logit_mult * jnp.dot(weights, texts, preferred_element_type=jnp.float32)
        grad_texts = grad_texts + logit_mult * jnp.dot(weights.T, left_rows, preferred_element_type=jnp.float32)
        return (grad_texts, loss_sum + loss_part), grad_left

    start_state = (jnp.zeros(texts.shape, jnp.float32), jnp.zeros((), jnp.float32))
    (grad_text, loss_sum), grad_blocks = lax.scan(block_step, start_state, jnp.arange(block_number, dtype=jnp.int32))
    grad_image = grad_blocks.reshape(pair_total, images.shape[1])
    return grad_image, grad_text, (loss_sum / pair_total).reshape(1)
```

```python
import jax
import jax.numpy as jnp
from jax import lax
from jax.sharding import Mesh
from jax.sharding import PartitionSpec as P

AXES = ("zh", "x", "zl", "y", "c")
PLANE = ("x", "y")
COLUMN = ("zh", "zl", "c")


def from_everyone(x, axes):
    size = lax.axis_size(axes)
    tiles = lax.all_to_all(jnp.broadcast_to(x[None], (size, *x.shape)), axes, 0, 0, tiled=True)
    return tiles.reshape(size * x.shape[0], *x.shape[1:])


def sent_and_summed(x, axes):
    size = lax.axis_size(axes)
    tiles = x.reshape(size, x.shape[0] // size, *x.shape[1:])
    return lax.all_to_all(tiles, axes, 0, 0, tiled=True).sum(axis=0)


def total(value, axes):
    size = lax.axis_size(axes)
    tile = jnp.broadcast_to(value, (size, 8, 128))
    return lax.all_to_all(tile, axes, 0, 0, tiled=True)[:, 0, 0].sum()


def shards(images, texts, logit_scale, logit_bias):
    rows = images.shape[0]
    multiplier = logit_scale[0]
    offset = logit_bias[0]
    left = from_everyone(images, PLANE)
    right = from_everyone(texts, COLUMN)
    logits = (
        lax.dot_general(left, right, (((1,), (1,)), ((), ())), preferred_element_type=jnp.float32)
        * multiplier
        + offset
    )
    left_ids = jnp.arange(left.shape[0], dtype=jnp.int32) - lax.axis_index(PLANE) * rows
    right_ids = jnp.arange(right.shape[0], dtype=jnp.int32) - lax.axis_index(COLUMN) * rows
    own = (left_ids >= 0) & (left_ids < rows)
    matched = (left_ids[:, None] == right_ids[None, :]) & own[:, None]
    weights = (jax.nn.sigmoid(logits) - matched.astype(jnp.float32)).astype(jnp.bfloat16)
    labels = jnp.where(matched, 1.0, -1.0).astype(jnp.float32)
    loss = -jnp.sum(jax.nn.log_sigmoid(labels * logits))
    grad_left = multiplier * jnp.dot(weights, right, preferred_element_type=jnp.float32)
    grad_right = multiplier * lax.dot_general(
        weights, left, (((0,), (0,)), ((), ())), preferred_element_type=jnp.float32
    )
    grad_image = sent_and_summed(grad_left, PLANE)
    grad_text = sent_and_summed(grad_right, COLUMN)
    loss = total(total(loss, PLANE), COLUMN)
    return (grad_image, grad_text, (loss / (rows * lax.axis_size(AXES))).reshape(1))


def solution(mesh):
    split = Mesh(mesh.devices.reshape(mesh.shape["grp"], 4, 2, 4, 2), AXES)
    in_specs = (P(AXES, None), P(AXES, None), P(), P())
    out_specs = (P(AXES, None), P(AXES, None), P())
    return jax.shard_map(
        shards, mesh=split, in_specs=in_specs, out_specs=out_specs, check_vma=False
    )
```

```python
import jax
import jax.numpy as jnp
from jax import lax
from jax.sharding import Mesh
from jax.sharding import PartitionSpec as P

AXES = ("zh", "x", "zl", "y", "c")
SIZES = (4, 4, 2, 4, 2)
PLANE = ("x", "y")
COLUMN = ("zh", "zl", "c")


def rank(zh, x, zl, y, c):
    return (((zh * 4 + x) * 2 + zl) * 4 + y) * 2 + c


def pairs(move):
    out = []
    for zh in range(4):
        for x in range(4):
            for zl in range(2):
                for y in range(4):
                    for c in range(2):
                        z2, x2, y2, c2 = move(zh * 2 + zl, x, y, c)
                        out.append(
                            (rank(zh, x, zl, y, c), rank(z2 % 8 // 2, x2 % 4, z2 % 2, y2 % 4, c2 % 2))
                        )
    return out


def step_first(d):
    return pairs(lambda z, x, y, c: (z, x + d * (1 - c), y + d * c, c))


def step_second(d):
    return pairs(lambda z, x, y, c: (z, x + d * c, y + d * (1 - c), c))


def step_z(d):
    return pairs(lambda z, x, y, c: (z + d, x, y, c))


def swap_core():
    return pairs(lambda z, x, y, c: (z, x, y, c + 1))


def send(x, perm):
    return lax.ppermute(x, AXES, perm)


def halves(x):
    n = x.shape[0] // 2
    return x[:n], x[n:]


def ring4_near(own, step):
    return send(own, step(1)), send(own, step(-1))


def ring4_far(left, right, step):
    return [send(halves(left)[0], step(1)), send(halves(right)[1], step(-1))]


def ring4_reduce_far(blocks, step):
    top, bottom = halves(blocks[3])
    return send(top, step(1)), send(bottom, step(-1))


def ring4_reduce_near(blocks, far, step):
    n = far[0].shape[0]
    to_left, to_right = blocks[1], blocks[2]
    to_right = jnp.concatenate([to_right[:n] + far[0], to_right[n:]])
    to_left = jnp.concatenate([to_left[:n], to_left[n:] + far[1]])
    return send(to_right, step(1)), send(to_left, step(-1))


def split(x, parts):
    n = x.shape[0] // parts
    return [x[i * n : (i + 1) * n] for i in range(parts)]


def total(value, axes):
    size = lax.axis_size(axes)
    tile = jnp.broadcast_to(value, (size, 8, 128))
    return lax.all_to_all(tile, axes, 0, 0, tiled=True)[:, 0, 0].sum()


def gathered(images, texts):
    left, right = ring4_near(images, step_first)
    below, above = send(texts, step_z(1)), send(texts, step_z(-1))
    column = [texts, below, above]
    far = ring4_far(left, right, step_first)
    below, above = send(below, step_z(1)), send(above, step_z(-1))
    column += [below, above]
    line = jnp.concatenate([images, left, right, *far])
    left, right = ring4_near(line, step_second)
    below, above = send(below, step_z(1)), send(above, step_z(-1))
    column += [below, above]
    far = ring4_far(left, right, step_second)
    column += [send(halves(below)[0], step_z(1)), send(halves(above)[1], step_z(-1))]
    plane = jnp.concatenate([line, left, right, *far])
    column = jnp.concatenate(column)
    column = jnp.concatenate([column, send(column, swap_core())])
    return plane, column


def reduced(grad_plane, grad_column):
    near, other = halves(grad_column)
    other = send(other, swap_core())
    blocks = split(grad_plane, 4)
    far = ring4_reduce_far(blocks, step_second)
    zs = split(near + other, 8)
    top, bottom = halves(zs[7])
    up, down = send(top, step_z(1)), send(bottom, step_z(-1))
    back = ring4_reduce_near(blocks, far, step_second)
    n = up.shape[0]
    up = jnp.concatenate([zs[6][:n] + up, zs[6][n:]])
    down = jnp.concatenate([zs[5][:n], zs[5][n:] + down])
    up, down = send(up, step_z(1)), send(down, step_z(-1))
    line = blocks[0] + back[0] + back[1]
    blocks = split(line, 4)
    far = ring4_reduce_far(blocks, step_first)
    up, down = send(zs[4] + up, step_z(1)), send(zs[3] + down, step_z(-1))
    back = ring4_reduce_near(blocks, far, step_first)
    up, down = send(zs[2] + up, step_z(1)), send(zs[1] + down, step_z(-1))
    return blocks[0] + back[0] + back[1], zs[0] + up + down


def shards(images, texts, logit_scale, logit_bias):
    rows = images.shape[0]
    multiplier = logit_scale[0]
    offset = logit_bias[0]
    left, right = gathered(images, texts)
    logits = (
        lax.dot_general(left, right, (((1,), (1,)), ((), ())), preferred_element_type=jnp.float32)
        * multiplier
        + offset
    )
    left_ids = jnp.arange(left.shape[0], dtype=jnp.int32)
    right_ids = jnp.arange(right.shape[0], dtype=jnp.int32)
    matched = (left_ids[:, None] == right_ids[None, :]) & (left_ids < rows)[:, None]
    weights = (jax.nn.sigmoid(logits) - matched.astype(jnp.float32)).astype(jnp.bfloat16)
    labels = jnp.where(matched, 1.0, -1.0).astype(jnp.float32)
    loss = -jnp.sum(jax.nn.log_sigmoid(labels * logits))
    grad_left = multiplier * jnp.dot(weights, right, preferred_element_type=jnp.float32)
    grad_right = multiplier * lax.dot_general(
        weights, left, (((0,), (0,)), ((), ())), preferred_element_type=jnp.float32
    )
    grad_image, grad_text = reduced(grad_left, grad_right)
    loss = total(total(loss, PLANE), COLUMN)
    return (grad_image, grad_text, (loss / (rows * lax.axis_size(AXES))).reshape(1))


def solution(mesh):
    split_mesh = Mesh(mesh.devices.reshape(mesh.shape["grp"], 4, 2, 4, 2), AXES)
    in_specs = (P(AXES, None), P(AXES, None), P(), P())
    out_specs = (P(AXES, None), P(AXES, None), P())
    return jax.shard_map(
        shards, mesh=split_mesh, in_specs=in_specs, out_specs=out_specs, check_vma=False
    )
```

```python
import jax
import jax.numpy as jnp
from jax import lax
from jax.sharding import Mesh
from jax.sharding import PartitionSpec as P

AXES = ("zh", "x", "zl", "y", "c")


def rank(zh, x, zl, y, c):
    return (((zh * 4 + x) * 2 + zl) * 4 + y) * 2 + c


def pairs(move):
    out = []
    for zh in range(4):
        for x in range(4):
            for zl in range(2):
                for y in range(4):
                    for c in range(2):
                        z2, x2, y2, c2 = move(zh * 2 + zl, x, y, c)
                        out.append(
                            (rank(zh, x, zl, y, c), rank(z2 % 8 // 2, x2 % 4, z2 % 2, y2 % 4, c2 % 2))
                        )
    return out


def step_first(d):
    return pairs(lambda z, x, y, c: (z, x + d * (1 - c), y + d * c, c))


def step_second(d):
    return pairs(lambda z, x, y, c: (z, x + d * c, y + d * (1 - c), c))


def step_z(d):
    return pairs(lambda z, x, y, c: (z + d, x, y, c))


def swap_core():
    return pairs(lambda z, x, y, c: (z, x, y, c + 1))


def send(x, perm):
    return lax.ppermute(x, AXES, perm)


def halves(x):
    n = x.shape[0] // 2
    return x[:n], x[n:]


def split(x, parts):
    n = x.shape[0] // parts
    return [x[i * n : (i + 1) * n] for i in range(parts)]


def gathered(images, texts):
    left, right, across = (send(images, step_first(d)) for d in (1, -1, 2))
    below1, above1, below2, above2 = (send(texts, step_z(d)) for d in (1, -1, 2, -2))
    line = jnp.concatenate([images, left, right, across])
    left, right = send(line, step_second(1)), send(line, step_second(-1))
    below3, above3 = send(below2, step_z(1)), send(above2, step_z(-1))
    top, bottom = send(halves(below2)[0], step_z(2)), send(halves(above2)[1], step_z(-2))
    far = send(halves(left)[0], step_second(1)), send(halves(right)[1], step_second(-1))
    column = jnp.concatenate([texts, below1, above1, below2, above2, below3, above3, top, bottom])
    plane = jnp.concatenate([line, left, right, *far])
    return plane, column, send(column, swap_core())


def added_at(block, piece, start):
    size = piece.shape[0]
    return lax.dynamic_update_slice(block, block[start : start + size] + piece, (start, 0))


TOTAL_MOVES = (
    lambda z, x, y, c: (z, x, y, c ^ 1),
    lambda z, x, y, c: (z, x ^ 1, y, c),
    lambda z, x, y, c: (z, x, y ^ 1, c),
    lambda z, x, y, c: (z ^ 1, x, y, c),
    lambda z, x, y, c: (z, x ^ 2, y, c),
    lambda z, x, y, c: (z, x, y ^ 2, c),
    lambda z, x, y, c: (z ^ 2, x, y, c),
    lambda z, x, y, c: (z ^ 4, x, y, c),
)


class Total:
    def __init__(self, value):
        self.tile = jnp.broadcast_to(value, (8, 128))
        self.count = 0
        self.move()

    def move(self):
        if self.count < len(TOTAL_MOVES):
            self.arriving = send(self.tile, pairs(TOTAL_MOVES[self.count]))
            self.count += 1
        else:
            self.arriving = None

    def after(self, *values):
        if self.arriving is None:
            return values
        self.tile, *values = lax.optimization_barrier((self.tile + self.arriving, *values))
        self.move()
        return values


def reduced(weights, images, texts, scale, total):
    def image_partial(start, stop):
        return scale * jnp.dot(weights[start:stop], texts, preferred_element_type=jnp.float32)

    def text_partial(start, stop):
        return scale * lax.dot_general(
            weights[:, start:stop], images, (((0,), (0,)), ((), ())), preferred_element_type=jnp.float32
        )

    n = weights.shape[0] // 8
    (other,) = total.after(text_partial(4 * n, 8 * n))
    other = send(other, swap_core())
    top, bottom = total.after(image_partial(6 * n, 7 * n), image_partial(7 * n, 8 * n))
    top, bottom = send(top, step_second(1)), send(bottom, step_second(-1))
    own_t, own_i = text_partial(0, 4 * n), image_partial(0, 2 * n)
    to_left, to_right = image_partial(2 * n, 4 * n), image_partial(4 * n, 6 * n)
    own_t, own_i, to_left, to_right = total.after(own_t, own_i, to_left, to_right)

    own_t, down1, up1, down2, up2, down3, up3, far = split(own_t + other, 8)
    z_top, z_bottom = halves(far)
    up3, down3, z_top, z_bottom = total.after(up3, down3, z_top, z_bottom)
    up3, down3 = send(up3, step_z(1)), send(down3, step_z(-1))
    z_top, z_bottom = send(z_top, step_z(2)), send(z_bottom, step_z(-2))
    up1, down1 = send(up1, step_z(1)), send(down1, step_z(-1))

    to_right, to_left = total.after(added_at(to_right, top, 0), added_at(to_left, bottom, n))
    to_right, to_left = send(to_right, step_second(1)), send(to_left, step_second(-1))

    up2 = added_at(up2 + up3, z_top, 0)
    down2 = added_at(down2 + down3, z_bottom, z_top.shape[0])
    up2, down2 = total.after(up2, down2)
    up2, down2 = send(up2, step_z(2)), send(down2, step_z(-2))

    own_i, to_left, to_right, across = total.after(*split(own_i + to_right + to_left, 4))
    to_left, to_right = send(to_left, step_first(-1)), send(to_right, step_first(1))
    across = send(across, step_first(2))
    (grad_text,) = total.after(own_t + up1 + down1 + up2 + down2)
    (grad_image,) = total.after(own_i + to_left + to_right + across)
    return grad_image, grad_text, total.tile[0, 0]


def shards(images, texts, logit_scale, logit_bias):
    rows = images.shape[0]
    multiplier = logit_scale[0]
    offset = logit_bias[0]
    plane, column, other = gathered(images, texts)
    texts_all = jnp.concatenate([column, other])
    logits = (
        lax.dot_general(
            plane, texts_all, (((1,), (1,)), ((), ())), preferred_element_type=jnp.float32
        )
        * multiplier
        + offset
    )
    plane_ids = jnp.arange(plane.shape[0], dtype=jnp.int32)
    text_ids = jnp.arange(texts_all.shape[0], dtype=jnp.int32)
    matched = (plane_ids[:, None] == text_ids[None, :]) & (plane_ids < rows)[:, None]
    weights = (jax.nn.sigmoid(logits) - matched.astype(jnp.float32)).astype(jnp.bfloat16)
    labels = jnp.where(matched, 1.0, -1.0).astype(jnp.float32)
    loss = -jnp.sum(jax.nn.log_sigmoid(labels * logits))
    weights, loss = lax.optimization_barrier((weights, loss))
    grad_image, grad_text, loss = reduced(weights, plane, texts_all, multiplier, Total(loss))
    return (grad_image, grad_text, (loss / (rows * lax.axis_size(AXES))).reshape(1))


def solution(mesh):
    split_mesh = Mesh(mesh.devices.reshape(mesh.shape["grp"], 4, 2, 4, 2), AXES)
    in_specs = (P(AXES, None), P(AXES, None), P(), P())
    out_specs = (P(AXES, None), P(AXES, None), P())
    return jax.shard_map(
        shards, mesh=split_mesh, in_specs=in_specs, out_specs=out_specs, check_vma=False
    )
```

```python
import jax
import jax.numpy as jnp
from jax import lax
from jax.sharding import Mesh
from jax.sharding import PartitionSpec as P

AXES = ("zh", "x", "zl", "y", "c")


def rank(zh, x, zl, y, c):
    return (((zh * 4 + x) * 2 + zl) * 4 + y) * 2 + c


def pairs(move):
    out = []
    for zh in range(4):
        for x in range(4):
            for zl in range(2):
                for y in range(4):
                    for c in range(2):
                        z2, x2, y2, c2 = move(zh * 2 + zl, x, y, c)
                        out.append(
                            (rank(zh, x, zl, y, c), rank(z2 % 8 // 2, x2, z2 % 2, y2, c2))
                        )
    return out


FIRST_A = pairs(lambda z, x, y, c: (z, x ^ (1 - c), y ^ c, c))
FIRST_B = pairs(lambda z, x, y, c: (z, x ^ 3 * (1 - c), y ^ 3 * c, c))
SECOND_A = pairs(lambda z, x, y, c: (z, x ^ c, y ^ (1 - c), c))
SECOND_B = pairs(lambda z, x, y, c: (z, x ^ 3 * c, y ^ 3 * (1 - c), c))
Z_A = pairs(lambda z, x, y, c: (z ^ 1, x, y, c))
Z_B = pairs(lambda z, x, y, c: (((z + 1) ^ 1) + 7, x, y, c))
CORE = pairs(lambda z, x, y, c: (z, x, y, c ^ 1))


def send(x, perm):
    return lax.ppermute(x, AXES, perm)


def halves(x):
    n = x.shape[0] // 2
    return x[:n], x[n:]


def split(x, parts):
    n = x.shape[0] // parts
    return [x[i * n : (i + 1) * n] for i in range(parts)]


def gathered(images, texts):
    a1, b1 = send(texts, Z_A), send(texts, Z_B)
    left, right = send(images, FIRST_A), send(images, FIRST_B)
    a2, b2 = send(b1, Z_A), send(a1, Z_B)
    far = send(halves(left)[0], FIRST_B), send(halves(right)[1], FIRST_A)
    line = jnp.concatenate([images, left, right, *far])
    a3, b3 = send(b2, Z_A), send(a2, Z_B)
    left, right = send(line, SECOND_A), send(line, SECOND_B)
    a4, b4 = send(halves(b3)[0], Z_A), send(halves(a3)[1], Z_B)
    far = send(halves(left)[0], SECOND_B), send(halves(right)[1], SECOND_A)
    column = jnp.concatenate([texts, a1, b1, a2, b2, a3, b3, a4, b4])
    plane = jnp.concatenate([line, left, right, *far])
    return plane, column, send(column, CORE)


def added_at(block, piece, start):
    size = piece.shape[0]
    return lax.dynamic_update_slice(block, block[start : start + size] + piece, (start, 0))


TOTAL_MOVES = (
    CORE,
    pairs(lambda z, x, y, c: (z, x ^ 1, y, c)),
    pairs(lambda z, x, y, c: (z, x, y ^ 1, c)),
    Z_A,
    pairs(lambda z, x, y, c: (z, x ^ 3, y, c)),
    pairs(lambda z, x, y, c: (z, x, y ^ 3, c)),
    Z_B,
    pairs(lambda z, x, y, c: (z + 4, x, y, c)),
)


class Total:
    def __init__(self, value):
        self.tile = jnp.broadcast_to(value, (8, 128))
        self.count = 0
        self.move()

    def move(self):
        if self.count < len(TOTAL_MOVES):
            self.arriving = send(self.tile, TOTAL_MOVES[self.count])
            self.count += 1
        else:
            self.arriving = None

    def after(self, *values):
        if self.arriving is None:
            return values
        self.tile, *values = lax.optimization_barrier((self.tile + self.arriving, *values))
        self.move()
        return values


def reduced(weights, images, texts, scale, total):
    def image_partial(start, stop):
        return scale * jnp.dot(weights[start:stop], texts, preferred_element_type=jnp.float32)

    def text_partial(start, stop):
        return scale * lax.dot_general(
            weights[:, start:stop], images, (((0,), (0,)), ((), ())), preferred_element_type=jnp.float32
        )

    n = weights.shape[0] // 8
    (other,) = total.after(text_partial(4 * n, 8 * n))
    other = send(other, CORE)
    far_a, far_b = total.after(image_partial(6 * n, 7 * n), image_partial(7 * n, 8 * n))
    far_a, far_b = send(far_a, SECOND_A), send(far_b, SECOND_B)
    own_t, own_i = text_partial(0, 4 * n), image_partial(0, 2 * n)
    to_a, to_b = image_partial(2 * n, 4 * n), image_partial(4 * n, 6 * n)
    own_t, own_i, to_a, to_b = total.after(own_t, own_i, to_a, to_b)

    own_t, a1, b1, a2, b2, a3, b3, z_far = split(own_t + other, 8)
    z_a, z_b = total.after(*halves(z_far))
    z_a, z_b = send(z_a, Z_A), send(z_b, Z_B)
    half = z_a.shape[0]

    to_a, to_b = total.after(added_at(to_a, far_b, n), added_at(to_b, far_a, 0))
    to_a, to_b = send(to_a, SECOND_A), send(to_b, SECOND_B)

    z_a, z_b = total.after(added_at(a3, z_b, half), added_at(b3, z_a, 0))
    z_a, z_b = send(z_a, Z_A), send(z_b, Z_B)
    z_a, z_b = total.after(a2 + z_b, b2 + z_a)
    z_a, z_b = send(z_a, Z_A), send(z_b, Z_B)

    own_i, to_a, to_b, far = split(own_i + to_a + to_b, 4)
    far_a, far_b = total.after(*halves(far))
    far_a, far_b = send(far_a, FIRST_A), send(far_b, FIRST_B)

    z_a, z_b = total.after(a1 + z_b, b1 + z_a)
    z_a, z_b = send(z_a, Z_A), send(z_b, Z_B)
    to_a, to_b = total.after(added_at(to_a, far_b, half), added_at(to_b, far_a, 0))
    to_a, to_b = send(to_a, FIRST_A), send(to_b, FIRST_B)
    (grad_text,) = total.after(own_t + z_a + z_b)
    (grad_image,) = total.after(own_i + to_a + to_b)
    return grad_image, grad_text, total.tile[0, 0]


def shards(images, texts, logit_scale, logit_bias):
    rows = images.shape[0]
    multiplier = logit_scale[0]
    offset = logit_bias[0]
    plane, column, other = gathered(images, texts)
    texts_all = jnp.concatenate([column, other])
    logits = (
        lax.dot_general(
            plane, texts_all, (((1,), (1,)), ((), ())), preferred_element_type=jnp.float32
        )
        * multiplier
        + offset
    )
    plane_ids = jnp.arange(plane.shape[0], dtype=jnp.int32)
    text_ids = jnp.arange(texts_all.shape[0], dtype=jnp.int32)
    matched = (plane_ids[:, None] == text_ids[None, :]) & (plane_ids < rows)[:, None]
    weights = (jax.nn.sigmoid(logits) - matched.astype(jnp.float32)).astype(jnp.bfloat16)
    labels = jnp.where(matched, 1.0, -1.0).astype(jnp.float32)
    loss = -jnp.sum(jax.nn.log_sigmoid(labels * logits))
    weights, loss = lax.optimization_barrier((weights, loss))
    grad_image, grad_text, loss = reduced(weights, plane, texts_all, multiplier, Total(loss))
    return (grad_image, grad_text, (loss / (rows * lax.axis_size(AXES))).reshape(1))


def solution(mesh):
    split_mesh = Mesh(mesh.devices.reshape(mesh.shape["grp"], 4, 2, 4, 2), AXES)
    in_specs = (P(AXES, None), P(AXES, None), P(), P())
    out_specs = (P(AXES, None), P(AXES, None), P())
    return jax.shard_map(
        shards, mesh=split_mesh, in_specs=in_specs, out_specs=out_specs, check_vma=False
    )
```

```python
import jax
import jax.numpy as jnp
from jax import lax
from jax.sharding import Mesh
from jax.sharding import PartitionSpec as P

AXES = ("zh", "x", "zl", "y", "c")


def rank(zh, x, zl, y, c):
    return (((zh * 4 + x) * 2 + zl) * 4 + y) * 2 + c


def pairs(move):
    out = []
    for zh in range(4):
        for x in range(4):
            for zl in range(2):
                for y in range(4):
                    for c in range(2):
                        z2, x2, y2, c2 = move(zh * 2 + zl, x, y, c)
                        out.append(
                            (rank(zh, x, zl, y, c), rank(z2 % 8 // 2, x2, z2 % 2, y2, c2))
                        )
    return out


FIRST_A = pairs(lambda z, x, y, c: (z, x ^ (1 - c), y ^ c, c))
FIRST_B = pairs(lambda z, x, y, c: (z, x ^ 3 * (1 - c), y ^ 3 * c, c))
SECOND_A = pairs(lambda z, x, y, c: (z, x ^ c, y ^ (1 - c), c))
SECOND_B = pairs(lambda z, x, y, c: (z, x ^ 3 * c, y ^ 3 * (1 - c), c))
Z_P = pairs(lambda z, x, y, c: (((z + c) ^ 1) - c, x, y, c))
Z_Q = pairs(lambda z, x, y, c: (((z + 1 - c) ^ 1) - 1 + c, x, y, c))
CORE = pairs(lambda z, x, y, c: (z, x, y, c ^ 1))


def send(x, perm):
    return lax.ppermute(x, AXES, perm)


def join(*parts):
    return jnp.concatenate(parts)


def gathered(images, texts):
    near = send(texts, Z_P)
    left = send(images, FIRST_A)
    pair = join(texts, near)
    z2 = send(pair, Z_Q)
    line1 = join(images, left)
    line2 = send(line1, FIRST_B)
    z3 = send(z2, Z_P)
    line1 = join(line1, send(line1, SECOND_A))
    line2 = join(line2, send(line2, SECOND_B))
    z4 = send(z3, Z_Q)
    plane = join(line1, send(line1, SECOND_B), line2, send(line2, SECOND_A))
    column = join(pair, z2, z3, z4)
    return plane, column, send(column, CORE)


TOTAL_MOVES = (
    pairs(lambda z, x, y, c: (z, x ^ 1, y, c)),
    pairs(lambda z, x, y, c: (z, x, y ^ 1, c)),
    pairs(lambda z, x, y, c: (z, x ^ 3, y, c)),
    pairs(lambda z, x, y, c: (z, x, y ^ 3, c)),
    pairs(lambda z, x, y, c: (z ^ 1, x, y, c)),
    CORE,
    pairs(lambda z, x, y, c: (((z + 1) ^ 1) - 1, x, y, c)),
    pairs(lambda z, x, y, c: (z + 4, x, y, c)),
)


class Total:
    def __init__(self, value):
        self.tile = jnp.broadcast_to(value, (8, 128))
        self.count = 0
        self.move()

    def move(self):
        if self.count < len(TOTAL_MOVES):
            self.arriving = send(self.tile, TOTAL_MOVES[self.count])
            self.count += 1
        else:
            self.arriving = None

    def after(self, *values):
        if self.arriving is None:
            return values
        self.tile, *values = lax.optimization_barrier((self.tile + self.arriving, *values))
        self.move()
        return values


def reduced(weights, images, texts, scale, total):
    def image_partial(start, stop):
        return scale * jnp.dot(weights[start:stop], texts, preferred_element_type=jnp.float32)

    def text_partial(start, stop):
        return scale * lax.dot_general(
            weights[:, start:stop], images, (((0,), (0,)), ((), ())), preferred_element_type=jnp.float32
        )

    n = weights.shape[0] // 8
    m = n // 2
    other = send(text_partial(4 * n, 8 * n), CORE)
    far1, far2 = send(image_partial(2 * n, 4 * n), SECOND_B), send(image_partial(6 * n, 8 * n), SECOND_A)
    pair, z2, z3, z4 = (text_partial(i * n, (i + 1) * n) for i in range(4))
    near1, near2 = image_partial(0, 2 * n), image_partial(4 * n, 6 * n)
    pair, z2, z3, z4, near1, near2 = total.after(pair, z2, z3, z4, near1, near2)

    (z4,) = total.after(z4 + other[3 * n :])
    z4 = send(z4, Z_Q)
    near1, near2 = total.after(near1 + far1, near2 + far2)
    far1, far2 = send(near1[n:], SECOND_A), send(near2[n:], SECOND_B)
    (z3,) = total.after(z3 + other[2 * n : 3 * n] + z4)
    z3 = send(z3, Z_P)
    (line2,) = total.after(near2[:n] + far2)
    line2 = send(line2, FIRST_B)
    (z2,) = total.after(z2 + other[n : 2 * n] + z3)
    z2 = send(z2, Z_Q)
    (line1,) = total.after(near1[:n] + far1 + line2)
    left = send(line1[m:], FIRST_A)
    (pair,) = total.after(pair + other[:n] + z2)
    near = send(pair[m:], Z_P)
    grad_image = line1[:m] + left
    grad_text = pair[:m] + near
    return grad_image, grad_text, total.tile[0, 0]


def shards(images, texts, logit_scale, logit_bias):
    rows = images.shape[0]
    multiplier = logit_scale[0]
    offset = logit_bias[0]
    plane, column, other = gathered(images, texts)
    texts_all = jnp.concatenate([column, other])
    logits = (
        lax.dot_general(
            plane, texts_all, (((1,), (1,)), ((), ())), preferred_element_type=jnp.float32
        )
        * multiplier
        + offset
    )
    plane_ids = jnp.arange(plane.shape[0], dtype=jnp.int32)
    text_ids = jnp.arange(texts_all.shape[0], dtype=jnp.int32)
    matched = (plane_ids[:, None] == text_ids[None, :]) & (plane_ids < rows)[:, None]
    weights = (jax.nn.sigmoid(logits) - matched.astype(jnp.float32)).astype(jnp.bfloat16)
    labels = jnp.where(matched, 1.0, -1.0).astype(jnp.float32)
    loss = -jnp.sum(jax.nn.log_sigmoid(labels * logits))
    weights, loss = lax.optimization_barrier((weights, loss))
    grad_image, grad_text, loss = reduced(weights, plane, texts_all, multiplier, Total(loss))
    return (grad_image, grad_text, (loss / (rows * lax.axis_size(AXES))).reshape(1))


def solution(mesh):
    split_mesh = Mesh(mesh.devices.reshape(mesh.shape["grp"], 4, 2, 4, 2), AXES)
    in_specs = (P(AXES, None), P(AXES, None), P(), P())
    out_specs = (P(AXES, None), P(AXES, None), P())
    return jax.shard_map(
        shards, mesh=split_mesh, in_specs=in_specs, out_specs=out_specs, check_vma=False
    )
```

```python
import jax
import jax.numpy as jnp
from jax import lax
from jax.sharding import Mesh
from jax.sharding import PartitionSpec as P

AXES = ("zh", "x", "zl", "y", "c")


def rank(zh, x, zl, y, c):
    return (((zh * 4 + x) * 2 + zl) * 4 + y) * 2 + c


def pairs(move):
    out = []
    for zh in range(4):
        for x in range(4):
            for zl in range(2):
                for y in range(4):
                    for c in range(2):
                        z2, x2, y2, c2 = move(zh * 2 + zl, x, y, c)
                        out.append(
                            (rank(zh, x, zl, y, c), rank(z2 % 8 // 2, x2, z2 % 2, y2, c2))
                        )
    return out


FIRST_A = pairs(lambda z, x, y, c: (z, x ^ (1 - c), y ^ c, c))
FIRST_B = pairs(lambda z, x, y, c: (z, x ^ 3 * (1 - c), y ^ 3 * c, c))
SECOND_A = pairs(lambda z, x, y, c: (z, x ^ c, y ^ (1 - c), c))
SECOND_B = pairs(lambda z, x, y, c: (z, x ^ 3 * c, y ^ 3 * (1 - c), c))
Z_P = pairs(lambda z, x, y, c: (((z + c) ^ 1) - c, x, y, c))
Z_Q = pairs(lambda z, x, y, c: (((z + 1 - c) ^ 1) - 1 + c, x, y, c))
CORE = pairs(lambda z, x, y, c: (z, x, y, c ^ 1))


def send(x, perm):
    return lax.ppermute(x, AXES, perm)


def join(*parts):
    return jnp.concatenate(parts)


def gathered(images, texts):
    near = send(texts, Z_P)
    left = send(images, FIRST_A)
    pair = join(texts, near)
    z2 = send(pair, Z_Q)
    line1 = join(images, left)
    line2 = send(line1, FIRST_B)
    z3 = send(z2, Z_P)
    line1 = join(line1, send(line1, SECOND_A))
    line2 = join(line2, send(line2, SECOND_B))
    z4 = send(z3, Z_Q)
    early = join(line1, line2)
    late = join(send(line1, SECOND_B), send(line2, SECOND_A))
    column = join(pair, z2, z3, z4)
    return early, late, join(column, send(column, CORE))


TOTAL_MOVES = (
    pairs(lambda z, x, y, c: (z ^ 1, x, y, c)),
    pairs(lambda z, x, y, c: (((z + 1) ^ 1) - 1, x, y, c)),
    pairs(lambda z, x, y, c: (z + 4, x, y, c)),
    CORE,
    pairs(lambda z, x, y, c: (z, x ^ 1, y, c)),
    pairs(lambda z, x, y, c: (z, x, y ^ 1, c)),
    pairs(lambda z, x, y, c: (z, x ^ 3, y, c)),
    pairs(lambda z, x, y, c: (z, x, y ^ 3, c)),
)


class Total:
    def __init__(self, value):
        self.tile = jnp.broadcast_to(value, (8, 128))
        self.count = 0
        self.move()

    def move(self):
        if self.count < len(TOTAL_MOVES):
            self.arriving = send(self.tile, TOTAL_MOVES[self.count])
            self.count += 1
        else:
            self.arriving = None

    def after(self, *values):
        if self.arriving is None:
            return values
        self.tile, *values = lax.optimization_barrier((self.tile + self.arriving, *values))
        self.move()
        return values


def logits_of(rows, texts, scale, offset):
    return (
        lax.dot_general(rows, texts, (((1,), (1,)), ((), ())), preferred_element_type=jnp.float32)
        * scale
        + offset
    )


def weights_and_loss(logits, matched=None):
    if matched is None:
        return jax.nn.sigmoid(logits).astype(jnp.bfloat16), -jnp.sum(jax.nn.log_sigmoid(-logits))
    weights = (jax.nn.sigmoid(logits) - matched.astype(jnp.float32)).astype(jnp.bfloat16)
    labels = jnp.where(matched, 1.0, -1.0).astype(jnp.float32)
    return weights, -jnp.sum(jax.nn.log_sigmoid(labels * logits))


def shards(images, texts, logit_scale, logit_bias):
    rows = images.shape[0]
    scale = logit_scale[0]
    offset = logit_bias[0]
    early, late, texts = gathered(images, texts)

    def image_partial(weights, start, stop):
        return scale * jnp.dot(weights[start:stop], texts, preferred_element_type=jnp.float32)

    def text_partial(weights, images, start, stop):
        return scale * lax.dot_general(
            weights[:, start:stop], images, (((0,), (0,)), ((), ())), preferred_element_type=jnp.float32
        )

    n = early.shape[0] // 4
    m = n // 2
    image_ids = jnp.arange(early.shape[0], dtype=jnp.int32)
    text_ids = jnp.arange(texts.shape[0], dtype=jnp.int32)
    matched = (image_ids[:, None] == text_ids[None, :]) & (image_ids < rows)[:, None]
    weights, loss = weights_and_loss(logits_of(early, texts, scale, offset), matched)
    weights, loss = lax.optimization_barrier((weights, loss))
    near1, near2 = image_partial(weights, 0, 2 * n), image_partial(weights, 2 * n, 4 * n)
    other_early = text_partial(weights, early, 4 * n, 8 * n)
    own_early = text_partial(weights, early, 0, 4 * n)
    near1, near2, other_early, own_early, late = lax.optimization_barrier(
        (near1, near2, other_early, own_early, late)
    )

    weights, loss_late = weights_and_loss(logits_of(late, texts, scale, offset))
    weights, loss = lax.optimization_barrier((weights, loss + loss_late))
    total = Total(loss)
    other = send(other_early + text_partial(weights, late, 4 * n, 8 * n), CORE)
    far1, far2 = total.after(image_partial(weights, 0, 2 * n), image_partial(weights, 2 * n, 4 * n))
    far1, far2 = send(far1, SECOND_B), send(far2, SECOND_A)
    pair, z2, z3, z4 = (
        own_early[i * n : (i + 1) * n] + text_partial(weights, late, i * n, (i + 1) * n)
        for i in range(4)
    )
    pair, z2, z3, z4 = total.after(pair, z2, z3, z4)

    (z4,) = total.after(z4 + other[3 * n :])
    z4 = send(z4, Z_Q)
    near1, near2 = total.after(near1 + far1, near2 + far2)
    far1, far2 = send(near1[n:], SECOND_A), send(near2[n:], SECOND_B)
    z3 = send(z3 + other[2 * n : 3 * n] + z4, Z_P)
    (line2,) = total.after(near2[:n] + far2)
    line2 = send(line2, FIRST_B)
    (z2,) = total.after(z2 + other[n : 2 * n] + z3)
    z2 = send(z2, Z_Q)
    (line1,) = total.after(near1[:n] + far1 + line2)
    left = send(line1[m:], FIRST_A)
    pair = pair + other[:n] + z2
    near = send(pair[m:], Z_P)
    grad_image = line1[:m] + left
    grad_text = pair[:m] + near
    total.after()
    return (grad_image, grad_text, (total.tile[0, 0] / (rows * lax.axis_size(AXES))).reshape(1))


def solution(mesh):
    split_mesh = Mesh(mesh.devices.reshape(mesh.shape["grp"], 4, 2, 4, 2), AXES)
    in_specs = (P(AXES, None), P(AXES, None), P(), P())
    out_specs = (P(AXES, None), P(AXES, None), P())
    return jax.shard_map(
        shards, mesh=split_mesh, in_specs=in_specs, out_specs=out_specs, check_vma=False
    )
```

```python
import jax
import jax.numpy as jnp
from jax import lax
from jax.sharding import Mesh
from jax.sharding import PartitionSpec as P


AXES = ("zh", "x", "zl", "y", "c")


def rank(zh, x, zl, y, c):
    return (((zh * 4 + x) * 2 + zl) * 4 + y) * 2 + c


def pairs(move):
    out = []
    for zh in range(4):
        for x in range(4):
            for zl in range(2):
                for y in range(4):
                    for c in range(2):
                        z2, x2, y2, c2 = move(zh * 2 + zl, x, y, c)
                        out.append(
                            (rank(zh, x, zl, y, c), rank(z2 % 8 // 2, x2, z2 % 2, y2, c2))
                        )
    return out


FIRST_A = pairs(lambda z, x, y, c: (z, x ^ (1 - c), y ^ c, c))
FIRST_B = pairs(lambda z, x, y, c: (z, x ^ 3 * (1 - c), y ^ 3 * c, c))
SECOND_A = pairs(lambda z, x, y, c: (z, x ^ c, y ^ (1 - c), c))
SECOND_B = pairs(lambda z, x, y, c: (z, x ^ 3 * c, y ^ 3 * (1 - c), c))
Z_P = pairs(lambda z, x, y, c: (((z + c) ^ 1) - c, x, y, c))
Z_Q = pairs(lambda z, x, y, c: (((z + 1 - c) ^ 1) - 1 + c, x, y, c))
CORE = pairs(lambda z, x, y, c: (z, x, y, c ^ 1))


def send(x, perm):
    return lax.ppermute(x, AXES, perm)


def join(*parts):
    return jnp.concatenate(parts)


def room(x):
    return lax.optimization_barrier(jnp.pad(x, ((0, x.shape[0]), (0, 0))))


def filled(x, rows):
    return lax.dynamic_update_slice(x, rows, (rows.shape[0], 0))


def gathered(images, texts):
    left = send(images, FIRST_A)
    near = send(texts, Z_P)
    line1 = filled(room(images), left)
    line2 = send(line1, FIRST_B)
    pair = filled(room(texts), near)
    z2 = send(pair, Z_Q)
    line1 = join(line1, send(line1, SECOND_A))
    line2 = join(line2, send(line2, SECOND_B))
    z3 = send(z2, Z_P)
    far1, far2 = send(line1, SECOND_B), send(line2, SECOND_A)
    z4 = send(z3, Z_Q)
    most = join(pair, z2, z3)
    most_other = send(most, CORE)
    other = join(most_other, send(z4, CORE))
    return join(line1, line2, far1, far2), join(most, z4, other)


TOTAL_MOVES = (
    pairs(lambda z, x, y, c: (z ^ 1, x, y, c)),
    pairs(lambda z, x, y, c: (((z + 1) ^ 1) - 1, x, y, c)),
    CORE,
    pairs(lambda z, x, y, c: (z + 4, x, y, c)),
    pairs(lambda z, x, y, c: (z, x ^ 1, y, c)),
    pairs(lambda z, x, y, c: (z, x, y ^ 1, c)),
    pairs(lambda z, x, y, c: (z, x ^ 3, y, c)),
    pairs(lambda z, x, y, c: (z, x, y ^ 3, c)),
)


def summed(value):
    tile = jnp.broadcast_to(value, (8, 128))
    for move in TOTAL_MOVES:
        tile = tile + send(tile, move)
    return tile[0, 0]


def logits_of(rows, texts, scale, offset):
    return (
        lax.dot_general(rows, texts, (((1,), (1,)), ((), ())), preferred_element_type=jnp.float32)
        * scale
        + offset
    )


def shards(images, texts, logit_scale, logit_bias):
    return step(images, texts, logit_scale[0], logit_bias[0])


def step(images, texts, scale, offset):
    rows = images.shape[0]
    plane, texts = gathered(images, texts)
    plane_ids = jnp.arange(plane.shape[0], dtype=jnp.int32)
    text_ids = jnp.arange(texts.shape[0], dtype=jnp.int32)
    matched = (plane_ids[:, None] == text_ids[None, :]) & (plane_ids < rows)[:, None]
    logits = logits_of(plane, texts, scale, offset)
    weights = (jax.nn.sigmoid(logits) - matched.astype(jnp.float32)).astype(jnp.bfloat16)
    labels = jnp.where(matched, 1.0, -1.0).astype(jnp.float32)
    loss = -jnp.sum(jax.nn.log_sigmoid(labels * logits))
    weights, loss = lax.optimization_barrier((weights, loss))

    def image_partial(start, stop):
        return scale * jnp.dot(weights[start:stop], texts, preferred_element_type=jnp.float32)

    def text_partial(start, stop):
        return scale * lax.dot_general(
            weights[:, start:stop], plane, (((0,), (0,)), ((), ())), preferred_element_type=jnp.float32
        )

    n = plane.shape[0] // 8
    m = n // 2
    last = text_partial(7 * n, 8 * n)
    last, weights = lax.optimization_barrier((last, weights))
    last = send(last, CORE)
    far1, far2 = image_partial(4 * n, 6 * n), image_partial(6 * n, 8 * n)
    far1, far2, weights = lax.optimization_barrier((far1, far2, weights))
    far1, far2 = send(far1, SECOND_B), send(far2, SECOND_A)
    other = send(text_partial(4 * n, 7 * n), CORE)
    total = summed(loss)
    pair, z2, z3, z4 = (text_partial(i * n, (i + 1) * n) for i in range(4))
    near1, near2 = image_partial(0, 2 * n), image_partial(2 * n, 4 * n)

    z4 = send(z4 + last, Z_Q)
    near1, near2 = near1 + far1, near2 + far2
    far1, far2 = send(near1[n:], SECOND_A), send(near2[n:], SECOND_B)
    z3 = send(z3 + other[2 * n : 3 * n] + z4, Z_P)
    line2 = send(near2[:n] + far2, FIRST_B)
    z2 = send(z2 + other[n : 2 * n] + z3, Z_Q)
    line1 = near1[:n] + far1 + line2
    left = send(line1[m:], FIRST_A)
    pair = pair + other[:n] + z2
    near = send(pair[m:], Z_P)
    grad_image = line1[:m] + left
    grad_text = pair[:m] + near
    return (grad_image, grad_text, (total / (rows * lax.axis_size(AXES))).reshape(1))


def solution(mesh):
    split_mesh = Mesh(mesh.devices.reshape(mesh.shape["grp"], 4, 2, 4, 2), AXES)
    in_specs = (P(AXES, None), P(AXES, None), P(), P())
    out_specs = (P(AXES, None), P(AXES, None), P())
    return jax.shard_map(
        shards, mesh=split_mesh, in_specs=in_specs, out_specs=out_specs, check_vma=False
    )
```

```python
import jax
import jax.numpy as jnp
from jax import lax
from jax.sharding import Mesh
from jax.sharding import PartitionSpec as P


AXES = ("zh", "x", "zl", "y", "c")


def rank(zh, x, zl, y, c):
    return (((zh * 4 + x) * 2 + zl) * 4 + y) * 2 + c


def pairs(move):
    out = []
    for zh in range(4):
        for x in range(4):
            for zl in range(2):
                for y in range(4):
                    for c in range(2):
                        z2, x2, y2, c2 = move(zh * 2 + zl, x, y, c)
                        out.append(
                            (rank(zh, x, zl, y, c), rank(z2 % 8 // 2, x2, z2 % 2, y2, c2))
                        )
    return out


FIRST_A = pairs(lambda z, x, y, c: (z, x ^ (1 - c), y ^ c, c))
FIRST_B = pairs(lambda z, x, y, c: (z, x ^ 3 * (1 - c), y ^ 3 * c, c))
SECOND_A = pairs(lambda z, x, y, c: (z, x ^ c, y ^ (1 - c), c))
SECOND_B = pairs(lambda z, x, y, c: (z, x ^ 3 * c, y ^ 3 * (1 - c), c))
Z_P = pairs(lambda z, x, y, c: (((z + c) ^ 1) - c, x, y, c))
Z_Q = pairs(lambda z, x, y, c: (((z + 1 - c) ^ 1) - 1 + c, x, y, c))
CORE = pairs(lambda z, x, y, c: (z, x, y, c ^ 1))


def send(x, perm):
    return lax.ppermute(x, AXES, perm)


def join(*parts):
    return jnp.concatenate(parts)


def room(x):
    return lax.optimization_barrier(jnp.pad(x, ((0, x.shape[0]), (0, 0))))


def filled(x, rows):
    return lax.dynamic_update_slice(x, rows, (rows.shape[0], 0))


def gathered(images, texts):
    left = send(images, FIRST_A)
    near = send(texts, Z_P)
    line1 = filled(room(images), left)
    line2 = send(line1, FIRST_B)
    pair = filled(room(texts), near)
    z2 = send(pair, Z_Q)
    line1 = join(line1, send(line1, SECOND_A))
    line2 = join(line2, send(line2, SECOND_B))
    z3 = send(z2, Z_P)
    far1, far2 = send(line1, SECOND_B), send(line2, SECOND_A)
    z4 = send(z3, Z_Q)
    most = join(pair, z2, z3)
    most_other = send(most, CORE)
    other = join(most_other, send(z4, CORE))
    return join(line1, line2, far1, far2), join(most, z4, other)


TOTAL_MOVES = (
    pairs(lambda z, x, y, c: (z ^ 1, x, y, c)),
    pairs(lambda z, x, y, c: (((z + 1) ^ 1) - 1, x, y, c)),
    CORE,
    pairs(lambda z, x, y, c: (z + 4, x, y, c)),
    pairs(lambda z, x, y, c: (z, x ^ 1, y, c)),
    pairs(lambda z, x, y, c: (z, x, y ^ 1, c)),
    pairs(lambda z, x, y, c: (z, x ^ 3, y, c)),
    pairs(lambda z, x, y, c: (z, x, y ^ 3, c)),
)


def summed(value):
    tile = jnp.broadcast_to(value, (8, 128))
    for step, move in enumerate(TOTAL_MOVES):
        arriving = send(tile, move)
        if step + 1 < len(TOTAL_MOVES):
            tile = tile + arriving
    return tile, arriving


def logits_of(rows, texts, scale, offset):
    return (
        lax.dot_general(rows, texts, (((1,), (1,)), ((), ())), preferred_element_type=jnp.float32)
        * scale
        + offset
    )


def shards(images, texts, logit_scale, logit_bias):
    return step(images, texts, logit_scale[0], logit_bias[0])


def step(images, texts, scale, offset):
    rows = images.shape[0]
    plane, texts = gathered(images, texts)
    plane_ids = jnp.arange(plane.shape[0], dtype=jnp.int32)
    text_ids = jnp.arange(texts.shape[0], dtype=jnp.int32)
    matched = (plane_ids[:, None] == text_ids[None, :]) & (plane_ids < rows)[:, None]
    logits = logits_of(plane, texts, scale, offset)
    weights = (jax.nn.sigmoid(logits) - matched.astype(jnp.float32)).astype(jnp.bfloat16)
    labels = jnp.where(matched, 1.0, -1.0).astype(jnp.float32)
    loss = -jnp.sum(jax.nn.log_sigmoid(labels * logits))
    weights, loss = lax.optimization_barrier((weights, loss))

    def image_partial(start, stop):
        return scale * jnp.dot(weights[start:stop], texts, preferred_element_type=jnp.float32)

    def text_partial(start, stop):
        return scale * lax.dot_general(
            weights[:, start:stop], plane, (((0,), (0,)), ((), ())), preferred_element_type=jnp.float32
        )

    n = plane.shape[0] // 8
    m = n // 2
    last = text_partial(7 * n, 8 * n)
    last, weights = lax.optimization_barrier((last, weights))
    last = send(last, CORE)
    far1, far2 = image_partial(4 * n, 6 * n), image_partial(6 * n, 8 * n)
    far1, far2, weights = lax.optimization_barrier((far1, far2, weights))
    far1, far2 = send(far1, SECOND_B), send(far2, SECOND_A)
    other = send(text_partial(4 * n, 7 * n), CORE)
    total = summed(loss)
    pair, z2, z3, z4 = (text_partial(i * n, (i + 1) * n) for i in range(4))
    near1, near2 = image_partial(0, 2 * n), image_partial(2 * n, 4 * n)

    z4 = send(z4 + last, Z_Q)
    near1, near2 = near1 + far1, near2 + far2
    far1, far2 = send(near1[n:], SECOND_A), send(near2[n:], SECOND_B)
    z3 = send(z3 + other[2 * n : 3 * n] + z4, Z_P)
    line2 = send(near2[:n] + far2, FIRST_B)
    z2 = send(z2 + other[n : 2 * n] + z3, Z_Q)
    line1 = near1[:n] + far1 + line2
    left = send(line1[m:], FIRST_A)
    pair = pair + other[:n] + z2
    near = send(pair[m:], Z_P)
    grad_image = line1[:m] + left
    grad_text = pair[:m] + near
    grad_image, grad_text, total = lax.optimization_barrier((grad_image, grad_text, total))
    total = (total[0] + total[1])[0, 0]
    return (grad_image, grad_text, (total / (rows * lax.axis_size(AXES))).reshape(1))


def solution(mesh):
    split_mesh = Mesh(mesh.devices.reshape(mesh.shape["grp"], 4, 2, 4, 2), AXES)
    in_specs = (P(AXES, None), P(AXES, None), P(), P())
    out_specs = (P(AXES, None), P(AXES, None), P())
    return jax.shard_map(
        shards, mesh=split_mesh, in_specs=in_specs, out_specs=out_specs, check_vma=False
    )
```
